32 devices in a mesh: rot: 8 (over z, y), cls: 4 (over x, core).
Axes of the slice: x: 2, y: 2, z: 4, core: 2. Of those that a mesh axis runs over, the one named last changes fastest.
Arguments:
- particles: bfloat16 [128, 16384], P('rot'), may hold values from -64 to 64
- references: bfloat16 [48, 96, 16384], P('cls', 'rot'), may hold values from -0.046875 to 0.046875
- micrograph: int32 [8, 16], P('rot'), may hold values from 0 to 3, never falling along the last dimension, each value on 1 to 8 neighbouring positions
- ctf: float32 [32, 64], P('rot'), may hold values from -1 to 1
- prior_class: int32 [128], P('rot'), may hold values from 0 to 47
Outputs:
- class_scores: float32 [128, 48], P('rot', 'cls')
- best_score: float32 [128], P('rot')
- prior_score: float32 [128], P('rot')
The draws below stay inside these ranges and needn't reach their ends.
Inputs may be any that keep to these rules, and one draw needn't show every extreme that they name: The entries of one row are the micrograph numbers of that index of rot in order, never falling; each of the 4 micrographs has 1 to 8 particles.
All inputs are finite; a program needn't handle non-finite values.
Results may differ from the reference program's by a relative error of at most 0.00095.
Values may be sent and summed in bfloat16 or wider, within the bound.
No kernel may reach another device: no remote copies, remote signals or barrier semaphores. Data moves between devices by JAX's collectives and lax.ppermute only.
A program may use at most 128 MiB of HBM per device.

```python
import math
import jax
import jax.numpy as jnp
import numpy as np
from jax import lax

CYCLES = 64
POLAR = 128
F = 16384
CLASSES = 48
ANGLES = 96
PART_DEV = 16
MICS_DEV = 4
MOST = 8
PARTICLES = 128
MICS = 32
N_ROT = 8


def draw_particles(key, part):
    first, second = jax.random.split(key, 2)
    base = jnp.clip(jax.random.normal(first, (PARTICLES, CYCLES, 2 * POLAR), jnp.float32), -6.0, 6.0)
    level = jnp.exp(jax.random.uniform(second, (PARTICLES, CYCLES, 1), jnp.float32, 0.0, math.log(10.0)))
    values = base * level
    values = jnp.clip(values, -64.0, 64.0)
    return values.reshape(PARTICLES, F).astype(jnp.bfloat16)


def place_ends(entries, own_key, smallest, top_value):
    extent = entries.shape
    place = [jax.random.randint(jax.random.fold_in(own_key, axis), (), 0, extent[axis]) for axis in range(len(extent))]
    entries = entries.at[tuple(place)].set(smallest)
    longest = extent.index(max(extent))
    place[longest] = (place[longest] + 1) % extent[longest]
    return entries.at[tuple(place)].set(top_value)


def levels(key, extent, cuts, low, top_value):
    level, own = 1.0, jax.random.fold_in(key, 6)
    for position, shards_of in cuts:
        steps = jnp.exp(jax.random.uniform(jax.random.fold_in(own, position), (shards_of,), jnp.float32, low / len(cuts), top_value / len(cuts)))
        level = level * jnp.repeat(steps, extent[position] // shards_of).reshape([-1 if axis == position else 1 for axis in range(len(extent))])
    return level


def split_up(count, total, limit, lean):
    portions = [(1 << 20) // math.isqrt(rank ** lean) + 1 for rank in range(2, count + 1)]
    surplus, given = total - limit - (count - 1), [1] * (count - 1)
    while surplus > 0:
        candidates = [i for i in range(count - 1) if given[i] < limit]
        mass, budget = sum([portions[i] for i in candidates]), surplus
        for i in candidates:
            addition = min(limit - given[i], max(1, budget * portions[i] // mass), surplus)
            given[i] = given[i] + addition
            surplus = surplus - addition
    return np.array([limit] + given)


def uneven(stream_key, amount, total, limit, slope):
    if amount == 2:
        one = jax.random.randint(stream_key, (), max(1, total - limit), min(limit, total - 1) + 1)
        return jnp.stack([one, total - one])
    sizes = jnp.asarray(split_up(amount, total, limit, slope), jnp.int32)
    pairs = (amount - 1) // 2
    donor, receiver = sizes[1:1 + 2 * pairs:2], sizes[2:2 + 2 * pairs:2]
    margin = jnp.minimum(donor - 1, limit - receiver)
    passed = jax.random.randint(jax.random.fold_in(stream_key, 1), (pairs,), 0, 1 << 20) % (margin + 1)
    sizes = sizes.at[1:1 + 2 * pairs:2].set(donor - passed).at[2:2 + 2 * pairs:2].set(receiver + passed)
    return sizes[jax.random.permutation(jax.random.fold_in(stream_key, 2), amount)]


def normal_values(stream_key, extent, deviation, reach, pieces=(), kind=jnp.bfloat16):
    loudness = levels(stream_key, extent, pieces, -0.22, 0.18) if pieces else 1.0
    drawn = jax.random.normal(stream_key, extent, jnp.float32) * deviation * loudness
    return jnp.minimum(jnp.maximum(drawn, -reach), reach).astype(kind)


def setup_inputs(seed: int = 0) -> dict:
    streams_of = jax.random.split(jax.random.key(seed), 6)
    particles = draw_particles(jax.random.fold_in(streams_of[5], 71), 0)
    references = normal_values(streams_of[1], (CLASSES, ANGLES, F), F ** -0.5, 0.046875, ((0, 4), (1, 8)))
    micrograph = jax.vmap(lambda own: jnp.searchsorted(jnp.cumsum(uneven(own, MICS_DEV, PART_DEV, MOST, 2)), jnp.arange(PART_DEV), side="right"))(jax.random.split(streams_of[2], N_ROT)).reshape((N_ROT, PART_DEV)).astype(jnp.int32)
    ctf = jnp.clip(jax.random.uniform(streams_of[3], (MICS, CYCLES), jnp.float32, -1.0, 1.0) * levels(streams_of[3], (MICS, CYCLES), ((0, 8),), -0.4, 0.0), -1.0, 1.0)
    prior_class = place_ends(jax.random.randint(streams_of[4], (PARTICLES,), 0, CLASSES), jax.random.fold_in(streams_of[4], 1), 0, CLASSES - 1).astype(jnp.int32)
    return dict(particles=particles, references=references, micrograph=micrograph, ctf=ctf, prior_class=prior_class)


def reference(particles, references, micrograph, ctf, prior_class):
    particle_spectra = particles.astype(jnp.float32).reshape(PARTICLES, CYCLES, 2 * POLAR)
    rotation_energy = lax.optimization_barrier(jnp.mean(particle_spectra * particle_spectra, axis=2)).reshape(N_ROT, PART_DEV, CYCLES)
    indicator_matrix = (micrograph[:, :, None] == jnp.arange(MICS_DEV, dtype=jnp.int32)[None, None, :]).astype(jnp.float32)
    score_totals = jnp.einsum('ekn,ekx->enx', indicator_matrix, rotation_energy, precision=lax.Precision.HIGHEST)
    counts = lax.optimization_barrier(jnp.sum(indicator_matrix, axis=1))
    mean_power = score_totals / counts[:, :, None]
    scaling_coefficient = ctf.reshape(N_ROT, MICS_DEV, CYCLES) * lax.rsqrt(mean_power + 1e-06)
    particle_scores = jnp.einsum('usn,uno->uso', indicator_matrix, scaling_coefficient, precision=lax.Precision.HIGHEST)
    particle_scores = particle_scores.reshape(PARTICLES, CYCLES)
    whitened = (particle_spectra * particle_scores[:, :, None]).reshape(PARTICLES, F).astype(jnp.bfloat16)

    def class_best(class_templates):
        scored = jnp.dot(class_templates, whitened.T, preferred_element_type=jnp.float32)
        return lax.optimization_barrier(jnp.max(scored, axis=0))
    per_class = lax.map(class_best, references)
    class_scores = per_class.T
    best_score = lax.optimization_barrier(jnp.max(class_scores, axis=1))
    prior_score = jnp.take_along_axis(class_scores, prior_class[:, None].astype(jnp.int32), axis=1)[:, 0]
    return (class_scores, best_score, prior_score)
```

```python
import functools

import jax
import jax.numpy as jnp
from jax import lax
from jax.experimental import pallas as pl
from jax.experimental.pallas import tpu as pltpu
from jax.sharding import PartitionSpec as P


EPS = 1e-06
NEG = -3.0e38
ROW = 16
GROUP = 8
MIB = 1 << 20

IN_SPECS = (P("rot", None), P("cls", "rot", None), P("rot", None), P("rot", None), P("rot"))
OUT_SPECS = (P("rot", "cls"), P("rot"), P("rot"))


def whiten_kernel(mic_ref, ctf_ref, p_ref, w_ref, q_ref, h_ref):
    n, features = p_ref.shape
    micros, cycles = ctf_ref.shape
    per = features // cycles
    lane = lax.broadcasted_iota(jnp.int32, (n, cycles), 1)
    power = jnp.zeros((n, cycles), jnp.float32)
    for r in range(cycles):
        x = p_ref[:, r * per : (r + 1) * per].astype(jnp.float32)
        power = jnp.where(lane == r, jnp.sum(x * x, axis=1, keepdims=True), power)
    power = power * (1.0 / per)
    row = lax.broadcasted_iota(jnp.int32, (n, n), 0)
    col = lax.broadcasted_iota(jnp.int32, (n, n), 1)
    mic = jnp.broadcast_to(mic_ref[...].astype(jnp.float32), (n, n))
    owner = jnp.sum(jnp.where(row == col, mic, 0.0), axis=1, keepdims=True)
    factor = jnp.zeros((n, cycles), jnp.float32)
    for m in range(micros):
        member = owner == float(m)
        count = jnp.sum(jnp.where(member, 1.0, 0.0), axis=0, keepdims=True)
        total = jnp.sum(jnp.where(member, power, 0.0), axis=0, keepdims=True)
        scale = ctf_ref[m : m + 1, :] * lax.rsqrt(total / count + EPS)
        factor = jnp.where(member, scale, factor)
    for r in range(cycles):
        part = slice(r * per, (r + 1) * per)
        x = p_ref[:, part].astype(jnp.float32)
        w_ref[:, part] = (x * factor[:, r : r + 1]).astype(jnp.bfloat16)
    cls = lax.axis_index("cls")
    quarter = q_ref.shape[1]
    q_ref[...] = w_ref[:, pl.ds(pl.multiple_of(cls * quarter, quarter), quarter)]
    half = h_ref.shape[1]
    h_ref[...] = w_ref[:, pl.ds(pl.multiple_of((cls % 2) * half, half), half)]


def score_kernel(steps, *refs):
    w_ref, y_ref, cy_ref, *rest = refs
    pieces, (r_ref, o_ref, all_ref) = rest[:-3], rest[-3:]
    n, features = w_ref.shape
    classes, angles, _ = r_ref.shape
    half, quarter = features // 2, features // 4
    rot, cls = lax.axis_index("rot"), lax.axis_index("cls")
    z, y, x, c = rot // 2, rot % 2, cls // 2, cls % 2

    def put(piece, zz, yy, at, size):
        rows = pl.ds(pl.multiple_of((zz * 2 + yy) * n, n), n)
        all_ref[rows, pl.ds(pl.multiple_of(at * size, size), size)] = piece[...]

    put(w_ref, z, y, 0, features)
    put(y_ref, z, 1 - y, c, half)
    put(cy_ref, z, 1 - y, 1 - c, half)
    for i, k in enumerate(steps):
        zk = jnp.bitwise_xor(z, k)
        for j, (yy, xx) in enumerate(((y, x), (y, 1 - x), (1 - y, x), (1 - y, 1 - x))):
            own, other = pieces[8 * i + 2 * j], pieces[8 * i + 2 * j + 1]
            put(own, zk, yy, 2 * xx + c, quarter)
            put(other, zk, yy, 2 * xx + 1 - c, quarter)

    total = all_ref.shape[0]
    score = jnp.zeros((classes * ROW, total), jnp.float32)
    block = quarter // 2
    for b in range(features // block):
        part = slice(b * block, (b + 1) * block)
        rows = r_ref[:, :, part]
        rows = jnp.concatenate(
            [rows, jnp.zeros((classes, ROW - angles, block), rows.dtype)], axis=1
        ).reshape(classes * ROW, block)
        score += lax.dot_general(
            rows, all_ref[:, part], (((1,), (1,)), ((), ())), preferred_element_type=jnp.float32
        )
    best = jnp.max(score.reshape(classes, ROW, total)[:, :angles], axis=1)
    best = jnp.concatenate([best, jnp.zeros((ROW - classes, total), jnp.float32)], axis=0)
    sub = lax.broadcasted_iota(jnp.int32, (GROUP, total), 0)
    lanes = lax.broadcasted_iota(jnp.int32, (GROUP, total), 1) // n
    copies = o_ref.shape[0] // (total // n)
    for g in range(ROW // GROUP):
        a = best[g * GROUP : (g + 1) * GROUP]
        chunk = jnp.zeros_like(a)
        for d in range(GROUP):
            moved = pltpu.roll(pltpu.roll(a, (GROUP - d) % GROUP, 0), d * n, 1)
            chunk = jnp.where(lanes == (sub + d) % GROUP, moved, chunk)
        for holder in range(total // n):
            for copy in range(copies):
                o_ref[holder * copies + copy, :, g * total : (g + 1) * total] = chunk[
                    holder : holder + 1
                ]


def final_kernel(holders, classes, in_ref, prior_ref, scores_ref, best_ref, chosen_ref):
    blocks = in_ref.shape[0] // holders
    width = in_ref.shape[2]
    n = prior_ref.shape[1]
    got = []
    for b in range(blocks):
        row = in_ref[b]
        for h in range(1, holders):
            row = jnp.maximum(row, in_ref[h * blocks + b])
        got.append(row)
    lane = lax.broadcasted_iota(jnp.int32, (1, width), 1)
    cls_of = lane // n
    real = cls_of < classes
    cls = lax.axis_index("cls")
    prior = jnp.concatenate([prior_ref[...]] * (width // n), axis=1)
    own = jnp.zeros((1, width), jnp.float32)
    top = jnp.full((1, width), NEG, jnp.float32)
    chosen = jnp.full((1, width), NEG, jnp.float32)
    for b in range(blocks):
        own = jnp.where(cls == b, got[b], own)
        top = jnp.maximum(top, jnp.where(real, got[b], NEG))
        hit = jnp.logical_and(real, prior == cls_of + b * classes)
        chosen = jnp.maximum(chosen, jnp.where(hit, got[b], NEG))

    def fold(v):
        size = width
        while size > n:
            size //= 2
            v = jnp.maximum(v[:, :size], v[:, size : 2 * size])
        return v

    best_ref[...] = fold(top)
    chosen_ref[...] = fold(chosen)
    at = lax.broadcasted_iota(jnp.int32, (n, width), 0)
    lanes = lax.broadcasted_iota(jnp.int32, (n, width), 1)
    spread = jnp.where(lanes % n == at, jnp.broadcast_to(own, (n, width)), 0.0)
    column = lax.broadcasted_iota(jnp.int32, (n, classes), 1)
    scores = jnp.zeros((n, classes), jnp.float32)
    for k in range(classes):
        one = jnp.sum(jnp.where(lanes // n == k, spread, 0.0), axis=1, keepdims=True)
        scores = jnp.where(column == k, one, scores)
    scores_ref[...] = scores


def direct_body(rots, parts, particles, references, micrograph, ctf, prior_class):
    n, features = particles.shape
    classes = references.shape[0]
    vmem = pl.BlockSpec(memory_space=pltpu.VMEM)
    bf16 = functools.partial(jax.ShapeDtypeStruct, dtype=jnp.bfloat16)
    f32 = functools.partial(jax.ShapeDtypeStruct, dtype=jnp.float32)

    def to(change):
        pairs = []
        for r in range(rots):
            for s in range(parts):
                z, y, x, c = change(r // 2, r % 2, s // 2, s % 2)
                pairs.append((r * parts + s, (z * 2 + y) * parts + x * 2 + c))
        return pairs

    def send(value, change):
        return lax.ppermute(value, ("rot", "cls"), to(change))

    def over_x(z, y, x, c):
        return z, y, 1 - x, c

    def over_y(z, y, x, c):
        return z, 1 - y, x, c

    def over_both(z, y, x, c):
        return z, 1 - y, 1 - x, c

    def over_core(z, y, x, c):
        return z, y, x, 1 - c

    whitened, quarter, half = pl.pallas_call(
        whiten_kernel,
        out_shape=(bf16((n, features)), bf16((n, features // 4)), bf16((n, features // 2))),
        in_specs=[vmem] * 3,
        out_specs=(vmem,) * 3,
    )(micrograph, ctf, particles)
    steps = tuple(range(1, rots // 2))
    got = {}
    got["y"] = send(half, over_y)
    for k in steps:
        got[f"z{k}"] = send(quarter, lambda z, y, x, c, k=k: (z ^ k, y, x, c))
    for k in steps:
        first = got[f"z{k}"]
        got[f"x{k}"] = send(first, over_x)
        got[f"y{k}"] = send(first, over_y)
        if k < 3:
            got[f"f{k}"] = send(got[f"y{k}"], over_x)
        else:
            got[f"f{k}"] = send(first, over_both)
    for name in list(got):
        got["c" + name] = send(got[name], over_core)
    pieces = []
    for k in steps:
        for kind in "zxyf":
            pieces += [got[f"{kind}{k}"], got[f"c{kind}{k}"]]
    chunks = pl.pallas_call(
        functools.partial(score_kernel, steps),
        out_shape=f32((rots * parts, 1, ROW * n)),
        in_specs=[vmem] * (len(pieces) + 4),
        out_specs=vmem,
        scratch_shapes=[pltpu.VMEM((rots * n, features), jnp.bfloat16)],
        compiler_params=pltpu.CompilerParams(vmem_limit_bytes=32 * MIB),
    )(whitened, got["y"], got["cy"], *pieces, references)
    received = lax.all_to_all(chunks, ("rot", "cls"), 0, 0, tiled=True)
    scores, best, chosen = pl.pallas_call(
        functools.partial(final_kernel, rots, classes),
        out_shape=(f32((n, classes)), f32((1, n)), f32((1, n))),
        in_specs=[vmem] * 2,
        out_specs=(vmem,) * 3,
    )(received, prior_class.reshape(1, n))
    return scores, best.reshape(n), chosen.reshape(n)


def gathered_body(particles, references, micrograph, ctf, prior_class):
    n, features = particles.shape
    micros, cycles = ctf.shape
    classes, angles, _ = references.shape
    rots = lax.axis_size("rot")
    spectra = particles.astype(jnp.float32).reshape(n, cycles, features // cycles)
    power = jnp.mean(spectra * spectra, axis=2)
    member = micrograph[0][:, None] == jnp.arange(micros, dtype=jnp.int32)[None, :]
    member = member.astype(jnp.float32)
    total = jnp.dot(member.T, power, precision=lax.Precision.HIGHEST)
    mean_power = total / jnp.sum(member, axis=0)[:, None]
    scale = ctf * lax.rsqrt(mean_power + EPS)
    factor = jnp.dot(member, scale, precision=lax.Precision.HIGHEST)
    whitened = (spectra * factor[:, :, None]).reshape(n, features).astype(jnp.bfloat16)
    table = references.reshape(classes * angles, features)
    everyone = lax.all_gather(whitened, "rot", axis=0, tiled=True)
    scored = lax.dot_general(
        table, everyone, (((1,), (1,)), ((), ())), preferred_element_type=jnp.float32
    )
    local = jnp.max(scored.reshape(classes, angles, everyone.shape[0]), axis=1)
    blocks = local.reshape(classes, rots, n)
    received = lax.all_to_all(blocks, "rot", split_axis=1, concat_axis=1, tiled=True)
    class_scores = jnp.max(received, axis=1).T
    local_best = jnp.max(class_scores, axis=1)
    index = lax.axis_index("cls") * classes + jnp.arange(classes, dtype=jnp.int32)
    chosen = prior_class[:, None] == index[None, :]
    local_prior = jnp.max(jnp.where(chosen, class_scores, -1e30), axis=1)
    best_score, prior_score = lax.pmax((local_best, local_prior), "cls")
    return class_scores, best_score, prior_score


def solution(mesh):
    rots, parts = mesh.shape["rot"], mesh.shape["cls"]
    few = rots == GROUP and parts == 4
    body = functools.partial(direct_body, rots, parts) if few else gathered_body
    return jax.shard_map(
        body, mesh=mesh, in_specs=IN_SPECS, out_specs=OUT_SPECS, check_vma=False
    )
```
